32 devices in a mesh: tm: 16 (over z, y, x), col: 2 (over core).
Axes of the slice: x: 2, y: 2, z: 4, core: 2. Of those that a mesh axis runs over, the one named last changes fastest.
Arguments:
- initial_state: float32 [1024], replicated, may hold values from -6 to 6
- coupling: float32 [1024, 1024], replicated, may hold values from -0.1875 to 0.1875
- modulation: float32 [1024, 1024], replicated, may hold values from -0.1875 to 0.1875
- gains: float32 [16, 5], P('tm'), may hold values from -1 to 1
- forcing: float32 [16, 5, 1024], P('tm'), may hold values from -6 to 6
Outputs:
- slab_ends: float32 [16, 1024], P('tm', 'col')
The draws below stay inside these ranges and needn't reach their ends.
All inputs are finite; a program needn't handle non-finite values.
Results may differ from the reference program's by a relative error of at most 0.0003.
Values sent between devices are 32-bit elements; how exact they have to be, the bound alone decides.
No kernel may reach another device: no remote copies, remote signals or barrier semaphores. Data moves between devices by JAX's collectives and lax.ppermute only.
A program may use at most 128 MiB of HBM per device.

```python
import jax
import jax.numpy as jnp
from jax import lax

D = 1024
STEPS = 2
NODES = 5
SLABS = 16


def block_scale(stream_key, dims, split, low, largest):
    def one(dim, parts):
        steps = jax.random.uniform(jax.random.fold_in(jax.random.fold_in(stream_key, 6), dim), (parts,), jnp.float32, low / len(split), largest / len(split))
        return jnp.repeat(jnp.exp(steps), dims[dim] // parts).reshape((-1,) + (1,) * (len(dims) - dim - 1))

    gain = one(*split[0])
    for cut in split[1:]:
        gain = gain * one(*cut)
    return gain


def gaussian(own_key, dims, width, limit, shards=(), kind=jnp.bfloat16):
    entries = jax.random.normal(own_key, dims, jnp.float32) * width
    if len(shards) > 0:
        entries = block_scale(own_key, dims, shards, -0.22, 0.18) * entries
    return jnp.clip(entries, min=-limit, max=limit).astype(kind)


def setup_inputs(seed: int = 0) -> dict:
    key_of = jax.random.split(jax.random.key(seed), 6)
    return {
        "initial_state": gaussian(key_of[0], (D,), 1.0, 6.0, (), jnp.float32),
        "coupling": gaussian(key_of[1], (D, D), D ** -0.5, 0.1875, (), jnp.float32),
        "modulation": gaussian(key_of[2], (D, D), D ** -0.5, 0.1875, (), jnp.float32),
        "gains": jnp.clip(jax.random.uniform(key_of[3], (SLABS, NODES), jnp.float32, -1.0, 1.0) * block_scale(key_of[3], (SLABS, NODES), ((0, 16),), -0.4, 0.0), -1.0, 1.0),
        "forcing": gaussian(key_of[4], (SLABS, NODES, D), 1.0, 6.0, ((0, 16),), jnp.float32),
    }


step_size = 0.1
highest = lax.Precision.HIGHEST


def apply_op(operator, current):
    return jnp.dot(operator, current, precision=highest)


def runge_step(current, op_start, op_mid, op_end, force_start, force_mid, force_end):
    slope_one = apply_op(op_start, current) + force_start
    slope_two = apply_op(op_mid, current + 0.5 * step_size * slope_one) + force_mid
    slope_three = apply_op(op_mid, current + 0.5 * step_size * slope_two) + force_mid
    slope_four = apply_op(op_end, current + step_size * slope_three) + force_end
    return current + (step_size / 6.0) * (slope_one + 2.0 * slope_two + 2.0 * slope_three + slope_four)


def reference(initial_state, coupling, modulation, gains, forcing):
    skew_base = coupling - coupling.T
    skew_vary = modulation - modulation.T

    def advance_slab(current, inputs):
        node_gain, node_force = inputs
        for substep in range(STEPS):
            op_start = skew_base + node_gain[2 * substep] * skew_vary
            op_mid = skew_base + node_gain[2 * substep + 1] * skew_vary
            op_end = skew_base + node_gain[2 * substep + 2] * skew_vary
            current = runge_step(current, op_start, op_mid, op_end, node_force[2 * substep], node_force[2 * substep + 1], node_force[2 * substep + 2])
        return current, current

    finished, slab_ends = lax.scan(advance_slab, initial_state, (gains, forcing))
    return slab_ends
```

```python
import jax
import jax.numpy as jnp
from jax import lax
from jax.experimental import pallas as pl
from jax.experimental.pallas import tpu as pltpu
from jax.sharding import PartitionSpec as P

step_size = 0.1
half = jnp.bfloat16
full = jnp.float32
tile = 256
min_cols = 64
spare_rows = 16


def group_span(state_size, time_parts, col_parts):
    span = max(1, state_size // (min_cols * col_parts))
    while span > 1 and (time_parts % span or state_size % (span * col_parts)):
        span -= 1
    return min(span, time_parts)


def split(value):
    high = value.astype(half)
    return high, (value - high.astype(full)).astype(half)


def panel_kernel(state_size, nodes, span, cols):
    rows = cols + spare_rows
    step_count = (nodes - 1) // 2
    blocks = state_size // tile

    def kernel(coupling, modulation, initial, slab_data, panels, base, vary, *splits):
        highs, lows = splits[:3], splits[3:]

        def build(source, target):
            for i in range(blocks):
                for j in range(i, blocks):
                    upper = source[i * tile:(i + 1) * tile, j * tile:(j + 1) * tile]
                    lower = source[j * tile:(j + 1) * tile, i * tile:(i + 1) * tile]
                    target[i * tile:(i + 1) * tile, j * tile:(j + 1) * tile] = lower.T - upper
                    if j > i:
                        target[j * tile:(j + 1) * tile, i * tile:(i + 1) * tile] = upper.T - lower

        build(coupling, base)
        build(modulation, vary)

        def form(slab, node, slot, begin, end):
            gain = slab_data[slab, nodes, node * 128:(node + 1) * 128].reshape(1, 128)
            gain = jnp.concatenate([gain] * (state_size // 128), axis=1)
            for row in range(begin, end, 128):
                value = base[row:row + 128, :] + gain * vary[row:row + 128, :]
                high, low = split(value)
                highs[slot][row:row + 128, :] = high
                lows[slot][row:row + 128, :] = low

        def apply_op(value, slot):
            high, low = split(value)
            both = jnp.concatenate([high, low], axis=0)
            main = jnp.dot(both, highs[slot][...], preferred_element_type=full)
            rest = jnp.dot(high, lows[slot][...], preferred_element_type=full)
            return main[:rows] + main[rows:] + rest

        row_ids = lax.broadcasted_iota(jnp.int32, (rows, state_size), 0)
        col_ids = lax.broadcasted_iota(jnp.int32, (rows, state_size), 1)
        time_index = lax.axis_index("tm")
        member = (time_index % span) * lax.axis_size("col") + lax.axis_index("col")
        start = jnp.where((row_ids + member * cols == col_ids) & (row_ids < cols), 1.0, 0.0)
        weight = jnp.where(time_index < span, 1.0, 0.0)
        start = start + jnp.where(row_ids == rows - 1, weight * initial[...], 0.0)
        is_last = jnp.where(lax.broadcasted_iota(jnp.int32, (rows, 1), 0) == rows - 1, 1.0, 0.0)

        slots = [2 if node == 0 else node % 2 for node in range(nodes)]
        form(0, 0, slots[0], 0, state_size)

        def slab_step(slab, current):
            def force(node):
                return is_last * slab_data[slab, node, :].reshape(1, state_size)

            for step in range(step_count):
                first, mid, last = 2 * step, 2 * step + 1, 2 * step + 2
                form(slab, mid, slots[mid], 0, state_size)
                slope_one = apply_op(current, slots[first]) + force(first)
                form(slab, last, slots[last], 0, state_size // 2)
                slope_two = apply_op(current + 0.5 * step_size * slope_one, slots[mid]) + force(mid)
                form(slab, last, slots[last], state_size // 2, state_size)
                slope_three = apply_op(current + 0.5 * step_size * slope_two, slots[mid]) + force(mid)
                if step == step_count - 1:
                    form(jnp.minimum(slab + 1, span - 1), 0, slots[0], 0, state_size)
                slope_four = apply_op(current + step_size * slope_three, slots[last]) + force(last)
                current = current + (step_size / 6.0) * (slope_one + 2.0 * slope_two + 2.0 * slope_three + slope_four)
            panels[pl.ds(slab, 1)] = current[None]
            return current

        lax.fori_loop(0, span, slab_step, start)

    vmem = pl.BlockSpec(memory_space=pltpu.VMEM)
    square = (state_size, state_size)
    return pl.pallas_call(
        kernel,
        out_shape=jax.ShapeDtypeStruct((span, rows, state_size), full),
        in_specs=[vmem] * 4,
        out_specs=vmem,
        scratch_shapes=[pltpu.VMEM(square, full)] * 2 + [pltpu.VMEM(square, half)] * 6,
        compiler_params=pltpu.CompilerParams(vmem_limit_bytes=60 * 1024 * 1024),
    )


def shards(initial_state, coupling, modulation, gains, forcing):
    state_size = coupling.shape[0]
    nodes = gains.shape[1]
    time_parts, col_parts = lax.axis_size("tm"), lax.axis_size("col")
    span = group_span(state_size, time_parts, col_parts)
    groups = time_parts // span
    members = span * col_parts
    cols = state_size // members
    time_index, col_index = lax.axis_index("tm"), lax.axis_index("col")
    group = time_index // span
    slab = time_index % span
    member = slab * col_parts + col_index
    teams = [[g * span + i for i in range(span)] for g in range(groups)]

    gain_row = jnp.pad(jnp.repeat(gains[0], 128), (0, state_size - nodes * 128))
    own = jnp.concatenate([forcing[0], gain_row[None]], axis=0)
    slab_data = lax.all_to_all(jnp.broadcast_to(own, (span,) + own.shape), "tm", 0, 0, axis_index_groups=teams)

    panels = panel_kernel(state_size, nodes, span, cols)(coupling, modulation, initial_state[None], slab_data)
    response = panels[:, -1, :]

    def own_cols(value):
        return lax.dynamic_slice_in_dim(value, member * cols, cols, 0)

    arrived = lax.ppermute(response[-1], "tm", [(i, (i + span) % time_parts) for i in range(time_parts)])
    begin = jnp.where(group == 1, own_cols(arrived), 0.0)
    for turn in range(1, groups - 1):
        partial = jnp.sum(panels[-1, :cols, :] * begin[:, None], axis=0)
        partial = partial + jnp.where(member == 0, 1.0, 0.0) * response[-1]
        outgoing = jnp.zeros((time_parts * col_parts, cols), full)
        outgoing = lax.dynamic_update_slice_in_dim(outgoing, partial.reshape(members, cols), ((group + 1) % groups) * members, 0)
        incoming = lax.all_to_all(outgoing, ("tm", "col"), 0, 0)
        begin = jnp.where(group == turn + 1, jnp.sum(incoming, axis=0), begin)

    partials = jnp.sum(panels[:, :cols, :] * begin[None, :, None], axis=1)
    received = lax.all_to_all(partials, "tm", 0, 0, axis_index_groups=teams)
    summed = jnp.sum(received, axis=0).reshape(col_parts, state_size // col_parts)
    slab_end = lax.psum_scatter(summed, "col", scatter_dimension=0) if col_parts != 2 else (
        lax.dynamic_index_in_dim(summed, col_index, 0, False)
        + lax.ppermute(lax.dynamic_index_in_dim(summed, 1 - col_index, 0, False), "col", [(0, 1), (1, 0)])
    )
    own_response = lax.dynamic_index_in_dim(response, slab, 0, False).reshape(col_parts, -1)
    slab_end = slab_end + lax.dynamic_index_in_dim(own_response, col_index, 0, False)
    return slab_end[None, :]


def solution(mesh):
    in_specs = (P(), P(), P(), P("tm", None), P("tm", None, None))
    out_specs = P("tm", "col")
    return jax.shard_map(shards, mesh=mesh, in_specs=in_specs, out_specs=out_specs, check_vma=False)
```

```python
import jax
import jax.numpy as jnp
from jax import lax
from jax.experimental import pallas as pl
from jax.experimental.pallas import tpu as pltpu
from jax.sharding import PartitionSpec as P

step_size = 0.1
half = jnp.bfloat16
full = jnp.float32
tile = 256
min_cols = 128
spare_rows = 16


def group_span(state_size, time_parts, col_parts):
    span = max(1, state_size // (min_cols * col_parts))
    while span > 1 and (time_parts % span or state_size % (span * col_parts)):
        span -= 1
    return min(span, time_parts)


def split(value):
    high = value.astype(half)
    return high, (value - high.astype(full)).astype(half)


def panel_kernel(state_size, nodes, span, cols):
    rows = cols + spare_rows
    step_count = (nodes - 1) // 2
    blocks = state_size // tile

    def kernel(coupling, modulation, initial, slab_data, panels, base, vary, *splits):
        highs, lows = splits[:3], splits[3:]

        def build(source, target):
            for i in range(blocks):
                for j in range(i, blocks):
                    upper = source[i * tile:(i + 1) * tile, j * tile:(j + 1) * tile]
                    lower = source[j * tile:(j + 1) * tile, i * tile:(i + 1) * tile]
                    target[i * tile:(i + 1) * tile, j * tile:(j + 1) * tile] = lower.T - upper
                    if j > i:
                        target[j * tile:(j + 1) * tile, i * tile:(i + 1) * tile] = upper.T - lower

        build(coupling, base)
        build(modulation, vary)

        def form(slab, node, slot, begin, end):
            gain = slab_data[slab, nodes, node * 128:(node + 1) * 128].reshape(1, 128)
            gain = jnp.concatenate([gain] * (state_size // 128), axis=1)
            for row in range(begin, end, 128):
                value = base[row:row + 128, :] + gain * vary[row:row + 128, :]
                high, low = split(value)
                highs[slot][row:row + 128, :] = high
                lows[slot][row:row + 128, :] = low

        def apply_op(value, slot):
            high, low = split(value)
            both = jnp.concatenate([high, low], axis=0)
            main = jnp.dot(both, highs[slot][...], preferred_element_type=full)
            rest = jnp.dot(high, lows[slot][...], preferred_element_type=full)
            return main[:rows] + main[rows:] + rest

        row_ids = lax.broadcasted_iota(jnp.int32, (rows, state_size), 0)
        col_ids = lax.broadcasted_iota(jnp.int32, (rows, state_size), 1)
        time_index = lax.axis_index("tm")
        member = (time_index % span) * lax.axis_size("col") + lax.axis_index("col")
        start = jnp.where((row_ids + member * cols == col_ids) & (row_ids < cols), 1.0, 0.0)
        weight = jnp.where(time_index < span, 1.0, 0.0)
        start = start + jnp.where(row_ids == rows - 1, weight * initial[...], 0.0)
        is_last = jnp.where(lax.broadcasted_iota(jnp.int32, (rows, 1), 0) == rows - 1, 1.0, 0.0)

        slots = [2 if node == 0 else node % 2 for node in range(nodes)]
        form(0, 0, slots[0], 0, state_size)

        def slab_step(slab, current):
            def force(node):
                return is_last * slab_data[slab, node, :].reshape(1, state_size)

            for step in range(step_count):
                first, mid, last = 2 * step, 2 * step + 1, 2 * step + 2
                form(slab, mid, slots[mid], 0, state_size)
                slope_one = apply_op(current, slots[first]) + force(first)
                form(slab, last, slots[last], 0, state_size // 2)
                slope_two = apply_op(current + 0.5 * step_size * slope_one, slots[mid]) + force(mid)
                form(slab, last, slots[last], state_size // 2, state_size)
                slope_three = apply_op(current + 0.5 * step_size * slope_two, slots[mid]) + force(mid)
                if step == step_count - 1:
                    form(jnp.minimum(slab + 1, span - 1), 0, slots[0], 0, state_size)
                slope_four = apply_op(current + step_size * slope_three, slots[last]) + force(last)
                current = current + (step_size / 6.0) * (slope_one + 2.0 * slope_two + 2.0 * slope_three + slope_four)
            panels[pl.ds(slab, 1)] = current[None]
            return current

        lax.fori_loop(0, span, slab_step, start)

    vmem = pl.BlockSpec(memory_space=pltpu.VMEM)
    square = (state_size, state_size)
    return pl.pallas_call(
        kernel,
        out_shape=jax.ShapeDtypeStruct((span, rows, state_size), full),
        in_specs=[vmem] * 4,
        out_specs=vmem,
        scratch_shapes=[pltpu.VMEM(square, full)] * 2 + [pltpu.VMEM(square, half)] * 6,
        compiler_params=pltpu.CompilerParams(vmem_limit_bytes=60 * 1024 * 1024),
    )


def shards(initial_state, coupling, modulation, gains, forcing):
    state_size = coupling.shape[0]
    nodes = gains.shape[1]
    time_parts, col_parts = lax.axis_size("tm"), lax.axis_size("col")
    span = group_span(state_size, time_parts, col_parts)
    groups = time_parts // span
    members = span * col_parts
    cols = state_size // members
    time_index, col_index = lax.axis_index("tm"), lax.axis_index("col")
    group = time_index // span
    slab = time_index % span
    member = slab * col_parts + col_index
    teams = [[g * span + i for i in range(span)] for g in range(groups)]

    gain_row = jnp.pad(jnp.repeat(gains[0], 128), (0, state_size - nodes * 128))
    own = jnp.concatenate([forcing[0], gain_row[None]], axis=0)
    slab_data = lax.all_to_all(jnp.broadcast_to(own, (span,) + own.shape), "tm", 0, 0, axis_index_groups=teams)

    panels = panel_kernel(state_size, nodes, span, cols)(coupling, modulation, initial_state[None], slab_data)
    response = panels[:, -1, :]

    def own_cols(value):
        return lax.dynamic_slice_in_dim(value, member * cols, cols, 0)

    arrived = lax.ppermute(response[-1], "tm", [(i, (i + span) % time_parts) for i in range(time_parts)])
    begin = jnp.where(group == 1, own_cols(arrived), 0.0)
    for turn in range(1, groups - 1):
        partial = jnp.sum(panels[-1, :cols, :] * begin[:, None], axis=0)
        partial = partial + jnp.where(member == 0, 1.0, 0.0) * response[-1]
        outgoing = jnp.zeros((time_parts * col_parts, cols), full)
        outgoing = lax.dynamic_update_slice_in_dim(outgoing, partial.reshape(members, cols), ((group + 1) % groups) * members, 0)
        incoming = lax.all_to_all(outgoing, ("tm", "col"), 0, 0)
        begin = jnp.where(group == turn + 1, jnp.sum(incoming, axis=0), begin)

    partials = jnp.sum(panels[:, :cols, :] * begin[None, :, None], axis=1)
    received = lax.all_to_all(partials, "tm", 0, 0, axis_index_groups=teams)
    summed = jnp.sum(received, axis=0).reshape(col_parts, state_size // col_parts)
    slab_end = lax.psum_scatter(summed, "col", scatter_dimension=0) if col_parts != 2 else (
        lax.dynamic_index_in_dim(summed, col_index, 0, False)
        + lax.ppermute(lax.dynamic_index_in_dim(summed, 1 - col_index, 0, False), "col", [(0, 1), (1, 0)])
    )
    own_response = lax.dynamic_index_in_dim(response, slab, 0, False).reshape(col_parts, -1)
    slab_end = slab_end + lax.dynamic_index_in_dim(own_response, col_index, 0, False)
    return slab_end[None, :]


def solution(mesh):
    in_specs = (P(), P(), P(), P("tm", None), P("tm", None, None))
    out_specs = P("tm", "col")
    return jax.shard_map(shards, mesh=mesh, in_specs=in_specs, out_specs=out_specs, check_vma=False)
```

```python
import jax
import jax.numpy as jnp
from jax import lax
from jax.experimental import pallas as pl
from jax.experimental.pallas import tpu as pltpu
from jax.sharding import PartitionSpec as P

step_size = 0.1
half = jnp.bfloat16
full = jnp.float32
tile = 256
min_cols = 128
spare_rows = 16


def group_span(state_size, time_parts, col_parts):
    span = max(1, state_size // (min_cols * col_parts))
    while span > 1 and (time_parts % span or state_size % (span * col_parts)):
        span -= 1
    return min(span, time_parts)


def split(value):
    high = value.astype(half)
    return high, (value - high.astype(full)).astype(half)


def panel_kernel(state_size, nodes, span, cols):
    rows = cols + spare_rows
    step_count = (nodes - 1) // 2
    blocks = state_size // tile

    def kernel(coupling, modulation, initial, slab_data, panels, responses, base, vary, *splits):
        highs, lows = splits[:3], splits[3:]

        def build(source, target):
            for i in range(blocks):
                for j in range(i, blocks):
                    upper = source[i * tile:(i + 1) * tile, j * tile:(j + 1) * tile]
                    lower = source[j * tile:(j + 1) * tile, i * tile:(i + 1) * tile]
                    target[i * tile:(i + 1) * tile, j * tile:(j + 1) * tile] = lower.T - upper
                    if j > i:
                        target[j * tile:(j + 1) * tile, i * tile:(i + 1) * tile] = upper.T - lower

        build(coupling, base)
        build(modulation, vary)

        def form(slab, node, slot, begin, end):
            gain = slab_data[slab, nodes, node * 128:(node + 1) * 128].reshape(1, 128)
            gain = jnp.concatenate([gain] * (state_size // 128), axis=1)
            for row in range(begin, end, 128):
                value = base[row:row + 128, :] + gain * vary[row:row + 128, :]
                high, low = split(value)
                highs[slot][row:row + 128, :] = high
                lows[slot][row:row + 128, :] = low

        def apply_op(value, slot):
            high, low = split(value)
            both = jnp.concatenate([high, low], axis=0)
            main = jnp.dot(both, highs[slot][...], preferred_element_type=full)
            rest = jnp.dot(high, lows[slot][...], preferred_element_type=full)
            return main[:rows] + main[rows:] + rest

        row_ids = lax.broadcasted_iota(jnp.int32, (rows, state_size), 0)
        col_ids = lax.broadcasted_iota(jnp.int32, (rows, state_size), 1)
        time_index = lax.axis_index("tm")
        member = (time_index % span) * lax.axis_size("col") + lax.axis_index("col")
        start = jnp.where((row_ids + member * cols == col_ids) & (row_ids < cols), 1.0, 0.0)
        weight = jnp.where(time_index < span, 1.0, 0.0)
        start = start + jnp.where(row_ids == rows - 1, weight * initial[...], 0.0)
        is_last = jnp.where(lax.broadcasted_iota(jnp.int32, (rows, 1), 0) == rows - 1, 1.0, 0.0)

        slots = [2 if node == 0 else node % 2 for node in range(nodes)]
        form(0, 0, slots[0], 0, state_size)

        def slab_step(slab, current):
            def force(node):
                return is_last * slab_data[slab, node, :].reshape(1, state_size)

            for step in range(step_count):
                first, mid, last = 2 * step, 2 * step + 1, 2 * step + 2
                form(slab, mid, slots[mid], 0, state_size)
                slope_one = apply_op(current, slots[first]) + force(first)
                form(slab, last, slots[last], 0, state_size // 2)
                slope_two = apply_op(current + 0.5 * step_size * slope_one, slots[mid]) + force(mid)
                form(slab, last, slots[last], state_size // 2, state_size)
                slope_three = apply_op(current + 0.5 * step_size * slope_two, slots[mid]) + force(mid)
                if step == step_count - 1:
                    form(jnp.minimum(slab + 1, span - 1), 0, slots[0], 0, state_size)
                slope_four = apply_op(current + step_size * slope_three, slots[last]) + force(last)
                current = current + (step_size / 6.0) * (slope_one + 2.0 * slope_two + 2.0 * slope_three + slope_four)
            panels[pl.ds(slab, 1)] = current[None, :cols]
            responses[pl.ds(slab, 1)] = current[None, rows - 1:rows]
            return current

        lax.fori_loop(0, span, slab_step, start)

    vmem = pl.BlockSpec(memory_space=pltpu.VMEM)
    square = (state_size, state_size)
    return pl.pallas_call(
        kernel,
        out_shape=[jax.ShapeDtypeStruct((span, count, state_size), full) for count in (cols, 1)],
        in_specs=[vmem] * 4,
        out_specs=[vmem] * 2,
        scratch_shapes=[pltpu.VMEM(square, full)] * 2 + [pltpu.VMEM(square, half)] * 6,
        compiler_params=pltpu.CompilerParams(vmem_limit_bytes=60 * 1024 * 1024),
    )


def weighted_rows(weights, panel):
    high, low = split(jnp.broadcast_to(weights, (16, weights.shape[1])))
    panel_high, panel_low = split(panel)
    total = jnp.dot(high, panel_high, preferred_element_type=full)
    total = total + jnp.dot(low, panel_high, preferred_element_type=full)
    return (total + jnp.dot(high, panel_low, preferred_element_type=full))[:1]


def hop_blocks(panels, responses, begin, share, members, copies):
    span, cols, state_size = panels.shape

    def kernel(weights, factor, panel, response, blocks):
        total = weighted_rows(weights[...], panel[0]) + factor[...] * response[0]
        for copy in range(copies):
            for member in range(members):
                blocks[copy * members + member] = total[:, member * cols:(member + 1) * cols]

    return pl.pallas_call(
        kernel,
        grid=(1,),
        out_shape=jax.ShapeDtypeStruct((copies * members, 1, cols), full),
        in_specs=[
            pl.BlockSpec((1, cols), lambda i: (0, 0)),
            pl.BlockSpec((1, state_size), lambda i: (0, 0)),
            pl.BlockSpec((1, cols, state_size), lambda i: (span - 1, 0, 0)),
            pl.BlockSpec((1, 1, state_size), lambda i: (span - 1, 0, 0)),
        ],
        out_specs=pl.BlockSpec((copies * members, 1, cols), lambda i: (0, 0, 0)),
    )(begin, share, panels, responses)


def slab_shares(panels, begin):
    span, cols, state_size = panels.shape

    def kernel(weights, panel, shares):
        shares[0] = weighted_rows(weights[...], panel[0])

    return pl.pallas_call(
        kernel,
        grid=(span,),
        out_shape=jax.ShapeDtypeStruct((span, 1, state_size), full),
        in_specs=[
            pl.BlockSpec((1, cols), lambda i: (0, 0)),
            pl.BlockSpec((1, cols, state_size), lambda i: (i, 0, 0)),
        ],
        out_specs=pl.BlockSpec((1, 1, state_size), lambda i: (i, 0, 0)),
    )(begin, panels)


def shards(initial_state, coupling, modulation, gains, forcing):
    state_size = coupling.shape[0]
    nodes = gains.shape[1]
    time_parts, col_parts = lax.axis_size("tm"), lax.axis_size("col")
    span = group_span(state_size, time_parts, col_parts)
    groups = time_parts // span
    members = span * col_parts
    cols = state_size // members
    time_index, col_index = lax.axis_index("tm"), lax.axis_index("col")
    group = time_index // span
    slab = time_index % span
    member = slab * col_parts + col_index
    teams = [[g * span + i for i in range(span)] for g in range(groups)]

    gain_row = jnp.pad(jnp.repeat(gains[0], 128), (0, state_size - nodes * 128))
    own = jnp.concatenate([forcing[0], gain_row[None]], axis=0)
    slab_data = lax.all_to_all(jnp.broadcast_to(own, (span,) + own.shape), "tm", 0, 0, axis_index_groups=teams)

    panels, responses = panel_kernel(state_size, nodes, span, cols)(coupling, modulation, initial_state[None], slab_data)

    if groups % 2 == 0:
        first_hop = [(i, i + span if i // span % 2 == 0 else i - span) for i in range(time_parts)]
    else:
        first_hop = [(i, (i + span) % time_parts) for i in range(time_parts)]
    arrived = lax.ppermute(responses[-1], "tm", first_hop)
    begin = lax.dynamic_slice_in_dim(arrived, member * cols, cols, 1)
    begin = jnp.where(group == 1, begin, 0.0)
    share = jnp.full((1, state_size), jnp.where(member == 0, 1.0, 0.0))
    source_group = jnp.arange(time_parts * col_parts).reshape(-1, 1, 1) // members
    for turn in range(1, groups - 1):
        outgoing = hop_blocks(panels, responses, begin, share, members, groups)
        incoming = lax.all_to_all(outgoing, ("tm", "col"), 0, 0, tiled=True)
        summed = jnp.sum(jnp.where(source_group == group - 1, incoming, 0.0), axis=0)
        begin = jnp.where(group == turn + 1, summed, begin)

    received = lax.all_to_all(slab_shares(panels, begin), "tm", 0, 0, axis_index_groups=teams, tiled=True)
    summed = jnp.sum(received, axis=0).reshape(col_parts, state_size // col_parts)
    slab_end = lax.psum_scatter(summed, "col", scatter_dimension=0) if col_parts != 2 else (
        lax.dynamic_index_in_dim(summed, col_index, 0, False)
        + lax.ppermute(lax.dynamic_index_in_dim(summed, 1 - col_index, 0, False), "col", [(0, 1), (1, 0)])
    )
    own_response = lax.dynamic_index_in_dim(responses, slab, 0, False).reshape(col_parts, -1)
    slab_end = slab_end + lax.dynamic_index_in_dim(own_response, col_index, 0, False)
    return slab_end[None, :]


def solution(mesh):
    in_specs = (P(), P(), P(), P("tm", None), P("tm", None, None))
    out_specs = P("tm", "col")
    return jax.shard_map(shards, mesh=mesh, in_specs=in_specs, out_specs=out_specs, check_vma=False)
```

```python
import jax
import jax.numpy as jnp
from jax import lax
from jax.experimental import pallas as pl
from jax.experimental.pallas import tpu as pltpu
from jax.sharding import PartitionSpec as P

step_size = 0.1
half = jnp.bfloat16
full = jnp.float32
tile = 256
min_cols = 128
spare_rows = 16


def group_span(state_size, time_parts, col_parts):
    span = max(1, state_size // (min_cols * col_parts))
    while span > 1 and (time_parts % span or state_size % (span * col_parts)):
        span -= 1
    return min(span, time_parts)


def split(value):
    high = value.astype(half)
    return high, (value - high.astype(full)).astype(half)


def panel_kernel(state_size, nodes, span, cols):
    rows = cols + spare_rows
    step_count = (nodes - 1) // 2
    blocks = state_size // tile

    def kernel(coupling, modulation, initial, slab_data, panels, responses, base, vary, *splits):
        highs, lows = splits[:3], splits[3:]

        def build(source, target):
            for i in range(blocks):
                for j in range(i, blocks):
                    upper = source[i * tile:(i + 1) * tile, j * tile:(j + 1) * tile]
                    lower = source[j * tile:(j + 1) * tile, i * tile:(i + 1) * tile]
                    target[i * tile:(i + 1) * tile, j * tile:(j + 1) * tile] = lower.T - upper
                    if j > i:
                        target[j * tile:(j + 1) * tile, i * tile:(i + 1) * tile] = upper.T - lower

        build(coupling, base)
        build(modulation, vary)

        def form(slab, node, slot, begin, end):
            gain = slab_data[slab, nodes, node * 128:(node + 1) * 128].reshape(1, 128)
            gain = jnp.concatenate([gain] * (state_size // 128), axis=1)
            for row in range(begin, end, 128):
                value = base[row:row + 128, :] + gain * vary[row:row + 128, :]
                high, low = split(value)
                highs[slot][row:row + 128, :] = high
                lows[slot][row:row + 128, :] = low

        def apply_op(value, slot):
            high, low = split(value)
            both = jnp.concatenate([high, low], axis=0)
            main = jnp.dot(both, highs[slot][...], preferred_element_type=full)
            rest = jnp.dot(high, lows[slot][...], preferred_element_type=full)
            return main[:rows] + main[rows:] + rest

        row_ids = lax.broadcasted_iota(jnp.int32, (rows, state_size), 0)
        col_ids = lax.broadcasted_iota(jnp.int32, (rows, state_size), 1)
        time_index = lax.axis_index("tm")
        member = (time_index % span) * lax.axis_size("col") + lax.axis_index("col")
        start = jnp.where((row_ids + member * cols == col_ids) & (row_ids < cols), 1.0, 0.0)
        weight = jnp.where(time_index < span, 1.0, 0.0)
        start = start + jnp.where(row_ids == rows - 1, weight * initial[...], 0.0)
        is_last = jnp.where(lax.broadcasted_iota(jnp.int32, (rows, 1), 0) == rows - 1, 1.0, 0.0)

        slots = [2 if node == 0 else node % 2 for node in range(nodes)]
        form(0, 0, slots[0], 0, state_size)

        def slab_step(slab, current):
            def force(node):
                return is_last * slab_data[slab, node, :].reshape(1, state_size)

            for step in range(step_count):
                first, mid, last = 2 * step, 2 * step + 1, 2 * step + 2
                form(slab, mid, slots[mid], 0, state_size)
                slope_one = apply_op(current, slots[first]) + force(first)
                form(slab, last, slots[last], 0, state_size // 2)
                slope_two = apply_op(current + 0.5 * step_size * slope_one, slots[mid]) + force(mid)
                form(slab, last, slots[last], state_size // 2, state_size)
                slope_three = apply_op(current + 0.5 * step_size * slope_two, slots[mid]) + force(mid)
                if step == step_count - 1:
                    form(jnp.minimum(slab + 1, span - 1), 0, slots[0], 0, state_size)
                slope_four = apply_op(current + step_size * slope_three, slots[last]) + force(last)
                current = current + (step_size / 6.0) * (slope_one + 2.0 * slope_two + 2.0 * slope_three + slope_four)
            panels[pl.ds(slab, 1)] = current[None, :cols]
            responses[pl.ds(slab, 1)] = current[None, rows - 1:rows]
            return current

        lax.fori_loop(0, span, slab_step, start)

    vmem = pl.BlockSpec(memory_space=pltpu.VMEM)
    square = (state_size, state_size)
    return pl.pallas_call(
        kernel,
        out_shape=[jax.ShapeDtypeStruct((span, count, state_size), full) for count in (cols, 1)],
        in_specs=[vmem] * 4,
        out_specs=[vmem] * 2,
        scratch_shapes=[pltpu.VMEM(square, full)] * 2 + [pltpu.VMEM(square, half)] * 6,
        compiler_params=pltpu.CompilerParams(vmem_limit_bytes=60 * 1024 * 1024),
    )


def team_gather(value, span, teams):
    count = value.shape[0]
    if span & (span - 1):
        copies = jnp.broadcast_to(value, (span,) + value.shape)
        return lax.all_to_all(copies, "tm", 0, 0, axis_index_groups=teams).reshape((span * count,) + value.shape[1:])
    place = lax.axis_index("tm") % span
    step = 1
    while step < span:
        other = lax.ppermute(value, "tm", [(i, i ^ step) for i in range(lax.axis_size("tm"))])
        is_upper = (place // step) % 2 == 1
        value = jnp.concatenate([jnp.where(is_upper, other, value), jnp.where(is_upper, value, other)], axis=0)
        step *= 2
    return value


def shards(initial_state, coupling, modulation, gains, forcing):
    state_size = coupling.shape[0]
    nodes = gains.shape[1]
    time_parts, col_parts = lax.axis_size("tm"), lax.axis_size("col")
    span = group_span(state_size, time_parts, col_parts)
    groups = time_parts // span
    members = span * col_parts
    cols = state_size // members
    time_index, col_index = lax.axis_index("tm"), lax.axis_index("col")
    group = time_index // span
    slab = time_index % span
    member = slab * col_parts + col_index
    teams = [[g * span + i for i in range(span)] for g in range(groups)]

    gain_row = jnp.pad(jnp.repeat(gains[0], 128), (0, state_size - nodes * 128))
    own = jnp.concatenate([forcing[0], gain_row[None]], axis=0)
    slab_data = team_gather(own[None], span, teams)

    panels, responses = panel_kernel(state_size, nodes, span, cols)(coupling, modulation, initial_state[None], slab_data)

    if groups % 2 == 0:
        first_hop = [(i, i + span if i // span % 2 == 0 else i - span) for i in range(time_parts)]
    else:
        first_hop = [(i, (i + span) % time_parts) for i in range(time_parts)]
    arrived = lax.ppermute(responses[-1], "tm", first_hop)
    begin = lax.dynamic_slice_in_dim(arrived[0], member * cols, cols, 0)
    begin = jnp.where(group == 1, begin, 0.0)
    source_group = jnp.arange(time_parts * col_parts).reshape(-1, 1, 1) // members
    for turn in range(1, groups - 1):
        partial = jnp.sum(panels[-1] * begin[:, None], axis=0)
        partial = partial + jnp.where(member == 0, responses[-1, 0], 0.0)
        outgoing = jnp.broadcast_to(partial.reshape(1, members, 1, cols), (groups, members, 1, cols)).reshape(-1, 1, cols)
        incoming = lax.all_to_all(outgoing, ("tm", "col"), 0, 0, tiled=True)
        summed = jnp.sum(jnp.where(source_group == group - 1, incoming, 0.0), axis=(0, 1))
        begin = jnp.where(group == turn + 1, summed, begin)

    partials = jnp.sum(panels * begin[None, :, None], axis=1)[:, None, :]
    received = lax.all_to_all(partials, "tm", 0, 0, axis_index_groups=teams, tiled=True)
    summed = jnp.sum(received, axis=0).reshape(col_parts, state_size // col_parts)
    slab_end = lax.psum_scatter(summed, "col", scatter_dimension=0) if col_parts != 2 else (
        lax.dynamic_index_in_dim(summed, col_index, 0, False)
        + lax.ppermute(lax.dynamic_index_in_dim(summed, 1 - col_index, 0, False), "col", [(0, 1), (1, 0)])
    )
    own_response = lax.dynamic_index_in_dim(responses, slab, 0, False).reshape(col_parts, -1)
    slab_end = slab_end + lax.dynamic_index_in_dim(own_response, col_index, 0, False)
    return slab_end[None, :]


def solution(mesh):
    in_specs = (P(), P(), P(), P("tm", None), P("tm", None, None))
    out_specs = P("tm", "col")
    return jax.shard_map(shards, mesh=mesh, in_specs=in_specs, out_specs=out_specs, check_vma=False)
```

```python
import jax
import jax.numpy as jnp
from jax import lax
from jax.experimental import pallas as pl
from jax.experimental.pallas import tpu as pltpu
from jax.sharding import PartitionSpec as P


step_size = 0.1
half = jnp.bfloat16
full = jnp.float32
tile = 256
min_cols = 128
spare_rows = 16


def group_span(state_size, time_parts, col_parts):
    span = max(1, state_size // (min_cols * col_parts))
    while span > 1 and (time_parts % span or state_size % (span * col_parts)):
        span -= 1
    return min(span, time_parts)


def split(value):
    high = value.astype(half)
    return high, (value - high.astype(full)).astype(half)


def panel_kernel(state_size, nodes, span, cols):
    rows = cols + spare_rows
    step_count = (nodes - 1) // 2
    blocks = state_size // tile

    def kernel(coupling, modulation, initial, slab_data, panels, responses, base, vary, *splits):
        highs, lows = splits[:3], splits[3:]

        def build(source, target):
            for i in range(blocks):
                for j in range(i, blocks):
                    upper = source[i * tile:(i + 1) * tile, j * tile:(j + 1) * tile]
                    lower = source[j * tile:(j + 1) * tile, i * tile:(i + 1) * tile]
                    target[i * tile:(i + 1) * tile, j * tile:(j + 1) * tile] = lower.T - upper
                    if j > i:
                        target[j * tile:(j + 1) * tile, i * tile:(i + 1) * tile] = upper.T - lower

        build(coupling, base)
        build(modulation, vary)

        def form(slab, node, slot, begin, end):
            gain = slab_data[slab, nodes, node * 128:(node + 1) * 128].reshape(1, 128)
            gain = jnp.concatenate([gain] * (state_size // 128), axis=1)
            for row in range(begin, end, 128):
                value = base[row:row + 128, :] + gain * vary[row:row + 128, :]
                high, low = split(value)
                highs[slot][row:row + 128, :] = high
                lows[slot][row:row + 128, :] = low

        def apply_op(value, slot):
            high, low = split(value)
            both = jnp.concatenate([high, low], axis=0)
            main = jnp.dot(both, highs[slot][...], preferred_element_type=full)
            rest = jnp.dot(high, lows[slot][...], preferred_element_type=full)
            return main[:rows] + main[rows:] + rest

        row_ids = lax.broadcasted_iota(jnp.int32, (rows, state_size), 0)
        col_ids = lax.broadcasted_iota(jnp.int32, (rows, state_size), 1)
        time_index = lax.axis_index("tm")
        member = (time_index % span) * lax.axis_size("col") + lax.axis_index("col")
        start = jnp.where((row_ids + member * cols == col_ids) & (row_ids < cols), 1.0, 0.0)
        weight = jnp.where(time_index < span, 1.0, 0.0)
        start = start + jnp.where(row_ids == rows - 1, weight * initial[...], 0.0)
        is_last = jnp.where(lax.broadcasted_iota(jnp.int32, (rows, 1), 0) == rows - 1, 1.0, 0.0)

        slots = [2 if node == 0 else node % 2 for node in range(nodes)]
        form(0, 0, slots[0], 0, state_size)

        def slab_step(slab, current):
            def force(node):
                return is_last * slab_data[slab, node, :].reshape(1, state_size)

            for step in range(step_count):
                first, mid, last = 2 * step, 2 * step + 1, 2 * step + 2
                form(slab, mid, slots[mid], 0, state_size)
                slope_one = apply_op(current, slots[first]) + force(first)
                form(slab, last, slots[last], 0, state_size // 2)
                slope_two = apply_op(current + 0.5 * step_size * slope_one, slots[mid]) + force(mid)
                form(slab, last, slots[last], state_size // 2, state_size)
                slope_three = apply_op(current + 0.5 * step_size * slope_two, slots[mid]) + force(mid)
                if step == step_count - 1:
                    form(jnp.minimum(slab + 1, span - 1), 0, slots[0], 0, state_size)
                slope_four = apply_op(current + step_size * slope_three, slots[last]) + force(last)
                current = current + (step_size / 6.0) * (slope_one + 2.0 * slope_two + 2.0 * slope_three + slope_four)
            panels[pl.ds(slab, 1)] = current[None, :cols]
            responses[pl.ds(slab, 1)] = current[None, rows - 1:rows]
            return current

        lax.fori_loop(0, span, slab_step, start)

    vmem = pl.BlockSpec(memory_space=pltpu.VMEM)
    square = (state_size, state_size)
    return pl.pallas_call(
        kernel,
        out_shape=[jax.ShapeDtypeStruct((span, count, state_size), full) for count in (cols, 1)],
        in_specs=[vmem] * 4,
        out_specs=[vmem] * 2,
        scratch_shapes=[pltpu.VMEM(square, full)] * 2 + [pltpu.VMEM(square, half)] * 6,
        compiler_params=pltpu.CompilerParams(vmem_limit_bytes=60 * 1024 * 1024),
    )


def partners(step):
    return [(i, i ^ step) for i in range(lax.axis_size("tm"))]


def team_gather(value, span, teams):
    if span & (span - 1):
        return lax.all_to_all(jnp.broadcast_to(value, (span,) + value.shape), "tm", 0, 0, axis_index_groups=teams)
    place = lax.axis_index("tm") % span
    values = [value] + [lax.ppermute(value, "tm", partners(step)) for step in range(1, span)]
    bit = 1
    while bit < span:
        is_upper = (place // bit) % 2 == 1
        values = [jnp.where(is_upper, values[k ^ bit], values[k]) for k in range(span)]
        bit *= 2
    return jnp.stack(values)


def team_sum(value, span, teams):
    if span & (span - 1):
        return jnp.sum(lax.all_to_all(value, "tm", 0, 0, axis_index_groups=teams), axis=0)
    place = lax.axis_index("tm") % span
    rows = [value[k] for k in range(span)]
    bit = 1
    while bit < span:
        is_upper = (place // bit) % 2 == 1
        rows = [jnp.where(is_upper, rows[k ^ bit], rows[k]) for k in range(span)]
        bit *= 2
    return rows[0] + sum(lax.ppermute(rows[step], "tm", partners(step)) for step in range(1, span))


def shards(initial_state, coupling, modulation, gains, forcing):
    state_size = coupling.shape[0]
    nodes = gains.shape[1]
    time_parts, col_parts = lax.axis_size("tm"), lax.axis_size("col")
    span = group_span(state_size, time_parts, col_parts)
    groups = time_parts // span
    members = span * col_parts
    cols = state_size // members
    time_index, col_index = lax.axis_index("tm"), lax.axis_index("col")
    group = time_index // span
    slab = time_index % span
    member = slab * col_parts + col_index
    teams = [[g * span + i for i in range(span)] for g in range(groups)]

    gain_row = jnp.pad(jnp.repeat(gains[0], 128), (0, state_size - nodes * 128))
    own = jnp.concatenate([forcing[0], gain_row[None]], axis=0)
    slab_data = team_gather(own, span, teams)

    panels, responses = panel_kernel(state_size, nodes, span, cols)(coupling, modulation, initial_state[None], slab_data)

    if groups % 2 == 0:
        first_hop = [(i, i + span if i // span % 2 == 0 else i - span) for i in range(time_parts)]
    else:
        first_hop = [(i, (i + span) % time_parts) for i in range(time_parts)]
    arrived = lax.ppermute(responses[-1], "tm", first_hop)
    begin = lax.dynamic_slice_in_dim(arrived[0], member * cols, cols, 0)
    begin = jnp.where(group == 1, begin, 0.0)
    source_group = jnp.arange(time_parts * col_parts).reshape(-1, 1, 1) // members
    for turn in range(1, groups - 1):
        partial = jnp.sum(panels[-1] * begin[:, None], axis=0)
        partial = partial + jnp.where(member == 0, responses[-1, 0], 0.0)
        outgoing = jnp.broadcast_to(partial.reshape(1, members, 1, cols), (groups, members, 1, cols)).reshape(-1, 1, cols)
        incoming = lax.all_to_all(outgoing, ("tm", "col"), 0, 0, tiled=True)
        summed = jnp.sum(jnp.where(source_group == group - 1, incoming, 0.0), axis=(0, 1))
        begin = jnp.where(group == turn + 1, summed, begin)

    partials = jnp.sum(panels * begin[None, :, None], axis=1)
    summed = team_sum(partials, span, teams).reshape(col_parts, state_size // col_parts)
    slab_end = lax.psum_scatter(summed, "col", scatter_dimension=0) if col_parts != 2 else (
        lax.dynamic_index_in_dim(summed, col_index, 0, False)
        + lax.ppermute(lax.dynamic_index_in_dim(summed, 1 - col_index, 0, False), "col", [(0, 1), (1, 0)])
    )
    own_response = lax.dynamic_index_in_dim(responses, slab, 0, False).reshape(col_parts, -1)
    slab_end = slab_end + lax.dynamic_index_in_dim(own_response, col_index, 0, False)
    return slab_end[None, :]


def solution(mesh):
    in_specs = (P(), P(), P(), P("tm", None), P("tm", None, None))
    out_specs = P("tm", "col")
    return jax.shard_map(shards, mesh=mesh, in_specs=in_specs, out_specs=out_specs, check_vma=False)
```

```python
import jax
import jax.numpy as jnp
from jax import lax
from jax.experimental import pallas as pl
from jax.experimental.pallas import tpu as pltpu
from jax.sharding import PartitionSpec as P


step_size = 0.1
half = jnp.bfloat16
full = jnp.float32
tile = 256
min_cols = 128
spare_rows = 16


def group_span(state_size, time_parts, col_parts):
    span = max(1, state_size // (min_cols * col_parts))
    while span > 1 and (time_parts % span or state_size % (span * col_parts)):
        span -= 1
    return min(span, time_parts)


def split(value):
    high = value.astype(half)
    return high, (value - high.astype(full)).astype(half)


def panel_kernel(state_size, nodes, span, cols):
    rows = cols + spare_rows
    step_count = (nodes - 1) // 2
    blocks = state_size // tile

    def kernel(coupling, modulation, initial, slab_data, panels, responses, ending, base, vary, *splits):
        highs, lows = splits[:3], splits[3:]

        def build(source, target):
            for i in range(blocks):
                for j in range(i, blocks):
                    upper = source[i * tile:(i + 1) * tile, j * tile:(j + 1) * tile]
                    lower = source[j * tile:(j + 1) * tile, i * tile:(i + 1) * tile]
                    target[i * tile:(i + 1) * tile, j * tile:(j + 1) * tile] = lower.T - upper
                    if j > i:
                        target[j * tile:(j + 1) * tile, i * tile:(i + 1) * tile] = upper.T - lower

        build(coupling, base)
        build(modulation, vary)

        def form(slab, node, slot, begin, end):
            place = nodes * state_size + node * 128
            gain = slab_data[slab, :, place:place + 128]
            gain = jnp.concatenate([gain] * (state_size // 128), axis=1)
            for row in range(begin, end, 128):
                value = base[row:row + 128, :] + gain * vary[row:row + 128, :]
                high, low = split(value)
                highs[slot][row:row + 128, :] = high
                lows[slot][row:row + 128, :] = low

        def apply_op(value, slot):
            high, low = split(value)
            both = jnp.concatenate([high, low], axis=0)
            main = jnp.dot(both, highs[slot][...], preferred_element_type=full)
            rest = jnp.dot(high, lows[slot][...], preferred_element_type=full)
            return main[:rows] + main[rows:] + rest

        row_ids = lax.broadcasted_iota(jnp.int32, (rows, state_size), 0)
        col_ids = lax.broadcasted_iota(jnp.int32, (rows, state_size), 1)
        time_index = lax.axis_index("tm")
        member = (time_index % span) * lax.axis_size("col") + lax.axis_index("col")
        start = jnp.where((row_ids + member * cols == col_ids) & (row_ids < cols), 1.0, 0.0)
        weight = jnp.where(time_index < span, 1.0, 0.0)
        start = start + jnp.where(row_ids == rows - 1, weight * initial[...], 0.0)
        is_last = jnp.where(lax.broadcasted_iota(jnp.int32, (rows, 1), 0) == rows - 1, 1.0, 0.0)

        slots = [2 if node == 0 else node % 2 for node in range(nodes)]
        form(0, 0, slots[0], 0, state_size)

        def slab_step(slab, current):
            def force(node):
                return is_last * slab_data[slab, :, node * state_size:(node + 1) * state_size]

            for step in range(step_count):
                first, mid, last = 2 * step, 2 * step + 1, 2 * step + 2
                form(slab, mid, slots[mid], 0, state_size)
                slope_one = apply_op(current, slots[first]) + force(first)
                form(slab, last, slots[last], 0, state_size // 2)
                slope_two = apply_op(current + 0.5 * step_size * slope_one, slots[mid]) + force(mid)
                form(slab, last, slots[last], state_size // 2, state_size)
                slope_three = apply_op(current + 0.5 * step_size * slope_two, slots[mid]) + force(mid)
                if step == step_count - 1:
                    form(jnp.minimum(slab + 1, span - 1), 0, slots[0], 0, state_size)
                slope_four = apply_op(current + step_size * slope_three, slots[last]) + force(last)
                current = current + (step_size / 6.0) * (slope_one + 2.0 * slope_two + 2.0 * slope_three + slope_four)
            panels[pl.ds(slab, 1)] = current[None, :cols]
            responses[pl.ds(slab, 1)] = current[None, rows - 1:rows]
            ending[...] = current[rows - 1:rows]
            return current

        lax.fori_loop(0, span, slab_step, start)

    vmem = pl.BlockSpec(memory_space=pltpu.VMEM)
    square = (state_size, state_size)
    return pl.pallas_call(
        kernel,
        out_shape=[jax.ShapeDtypeStruct((span, count, state_size), full) for count in (cols, 1)]
        + [jax.ShapeDtypeStruct((1, state_size), full)],
        in_specs=[vmem] * 4,
        out_specs=[vmem] * 3,
        scratch_shapes=[pltpu.VMEM(square, full)] * 2 + [pltpu.VMEM(square, half)] * 6,
        compiler_params=pltpu.CompilerParams(vmem_limit_bytes=60 * 1024 * 1024),
    )


def partners(step):
    return [(i, i ^ step) for i in range(lax.axis_size("tm"))]


def team_gather(value, span, teams):
    if span & (span - 1):
        return lax.all_to_all(jnp.broadcast_to(value, (span,) + value.shape), "tm", 0, 0, axis_index_groups=teams)
    place = lax.axis_index("tm") % span
    values = [value] + [lax.ppermute(value, "tm", partners(step)) for step in range(1, span)]
    bit = 1
    while bit < span:
        is_upper = (place // bit) % 2 == 1
        values = [jnp.where(is_upper, values[k ^ bit], values[k]) for k in range(span)]
        bit *= 2
    return jnp.stack(values)


def team_sum(value, span, teams):
    if span & (span - 1):
        return jnp.sum(lax.all_to_all(value, "tm", 0, 0, axis_index_groups=teams), axis=0)
    place = lax.axis_index("tm") % span
    rows = [value[k] for k in range(span)]
    bit = 1
    while bit < span:
        is_upper = (place // bit) % 2 == 1
        rows = [jnp.where(is_upper, rows[k ^ bit], rows[k]) for k in range(span)]
        bit *= 2
    return rows[0] + sum(lax.ppermute(rows[step], "tm", partners(step)) for step in range(1, span))


def shards(initial_state, coupling, modulation, gains, forcing):
    state_size = coupling.shape[0]
    nodes = gains.shape[1]
    time_parts, col_parts = lax.axis_size("tm"), lax.axis_size("col")
    span = group_span(state_size, time_parts, col_parts)
    groups = time_parts // span
    members = span * col_parts
    cols = state_size // members
    time_index, col_index = lax.axis_index("tm"), lax.axis_index("col")
    group = time_index // span
    slab = time_index % span
    member = slab * col_parts + col_index
    teams = [[g * span + i for i in range(span)] for g in range(groups)]

    gain_row = jnp.pad(jnp.repeat(gains[0], 128), (0, state_size - nodes * 128))
    own = jnp.concatenate([forcing.reshape(-1), gain_row])
    slab_data = team_gather(own, span, teams)[:, None, :]

    panels, responses, ending = panel_kernel(state_size, nodes, span, cols)(coupling, modulation, initial_state[None], slab_data)

    if groups % 2 == 0:
        first_hop = [(i, i + span if i // span % 2 == 0 else i - span) for i in range(time_parts)]
    else:
        first_hop = [(i, (i + span) % time_parts) for i in range(time_parts)]
    arrived = lax.ppermute(ending, "tm", first_hop)
    begin = lax.dynamic_slice_in_dim(arrived[0], member * cols, cols, 0)
    begin = jnp.where(group == 1, begin, 0.0)
    source_group = jnp.arange(time_parts * col_parts).reshape(-1, 1, 1) // members
    for turn in range(1, groups - 1):
        partial = jnp.sum(panels[-1] * begin[:, None], axis=0)
        partial = partial + jnp.where(member == 0, ending[0], 0.0)
        outgoing = jnp.broadcast_to(partial.reshape(1, members, 1, cols), (groups, members, 1, cols)).reshape(-1, 1, cols)
        incoming = lax.all_to_all(outgoing, ("tm", "col"), 0, 0, tiled=True)
        summed = jnp.sum(jnp.where(source_group == group - 1, incoming, 0.0), axis=(0, 1))
        begin = jnp.where(group == turn + 1, summed, begin)

    partials = jnp.sum(panels * begin[None, :, None], axis=1)
    summed = team_sum(partials, span, teams).reshape(col_parts, state_size // col_parts)
    slab_end = lax.psum_scatter(summed, "col", scatter_dimension=0) if col_parts != 2 else (
        lax.dynamic_index_in_dim(summed, col_index, 0, False)
        + lax.ppermute(lax.dynamic_index_in_dim(summed, 1 - col_index, 0, False), "col", [(0, 1), (1, 0)])
    )
    own_response = lax.dynamic_index_in_dim(responses, slab, 0, False).reshape(col_parts, -1)
    slab_end = slab_end + lax.dynamic_index_in_dim(own_response, col_index, 0, False)
    return slab_end[None, :]


def solution(mesh):
    in_specs = (P(), P(), P(), P("tm", None), P("tm", None, None))
    out_specs = P("tm", "col")
    return jax.shard_map(shards, mesh=mesh, in_specs=in_specs, out_specs=out_specs, check_vma=False)
```

```python
import jax
import jax.numpy as jnp
from jax import lax
from jax.experimental import pallas as pl
from jax.experimental.pallas import tpu as pltpu
from jax.sharding import PartitionSpec as P


step_size = 0.1
half = jnp.bfloat16
full = jnp.float32
tile = 256
min_cols = 128
spare_rows = 16


def group_span(state_size, time_parts, col_parts):
    span = max(1, state_size // (min_cols * col_parts))
    while span > 1 and (time_parts % span or state_size % (span * col_parts)):
        span -= 1
    return min(span, time_parts)


def split(value):
    high = value.astype(half)
    return high, (value - high.astype(full)).astype(half)


def panel_kernel(state_size, nodes, span, cols):
    rows = cols + spare_rows
    step_count = (nodes - 1) // 2
    blocks = state_size // tile

    def kernel(coupling, modulation, initial, slab_data, panels, responses, ending, base, vary, *splits):
        highs, lows = splits[:3], splits[3:]

        def build(source, target):
            for i in range(blocks):
                for j in range(i, blocks):
                    upper = source[i * tile:(i + 1) * tile, j * tile:(j + 1) * tile]
                    lower = source[j * tile:(j + 1) * tile, i * tile:(i + 1) * tile]
                    target[i * tile:(i + 1) * tile, j * tile:(j + 1) * tile] = lower.T - upper
                    if j > i:
                        target[j * tile:(j + 1) * tile, i * tile:(i + 1) * tile] = upper.T - lower

        build(coupling, base)
        build(modulation, vary)

        def form(slab, node, slot, begin, end):
            gain = slab_data[slab, nodes, node * 128:(node + 1) * 128].reshape(1, 128)
            gain = jnp.concatenate([gain] * (state_size // 128), axis=1)
            for row in range(begin, end, 128):
                value = base[row:row + 128, :] + gain * vary[row:row + 128, :]
                high, low = split(value)
                highs[slot][row:row + 128, :] = high
                lows[slot][row:row + 128, :] = low

        def apply_op(value, slot):
            high, low = split(value)
            both = jnp.concatenate([high, low], axis=0)
            main = jnp.dot(both, highs[slot][...], preferred_element_type=full)
            rest = jnp.dot(high, lows[slot][...], preferred_element_type=full)
            return main[:rows] + main[rows:] + rest

        row_ids = lax.broadcasted_iota(jnp.int32, (rows, state_size), 0)
        col_ids = lax.broadcasted_iota(jnp.int32, (rows, state_size), 1)
        time_index = lax.axis_index("tm")
        member = (time_index % span) * lax.axis_size("col") + lax.axis_index("col")
        start = jnp.where((row_ids + member * cols == col_ids) & (row_ids < cols), 1.0, 0.0)
        weight = jnp.where(time_index < span, 1.0, 0.0)
        start = start + jnp.where(row_ids == rows - 1, weight * initial[...], 0.0)
        is_last = jnp.where(lax.broadcasted_iota(jnp.int32, (rows, 1), 0) == rows - 1, 1.0, 0.0)

        slots = [2 if node == 0 else node % 2 for node in range(nodes)]
        form(0, 0, slots[0], 0, state_size)

        def slab_step(slab, current):
            def force(node):
                return is_last * slab_data[slab, node, :].reshape(1, state_size)

            for step in range(step_count):
                first, mid, last = 2 * step, 2 * step + 1, 2 * step + 2
                form(slab, mid, slots[mid], 0, state_size)
                slope_one = apply_op(current, slots[first]) + force(first)
                form(slab, last, slots[last], 0, state_size // 2)
                slope_two = apply_op(current + 0.5 * step_size * slope_one, slots[mid]) + force(mid)
                form(slab, last, slots[last], state_size // 2, state_size)
                slope_three = apply_op(current + 0.5 * step_size * slope_two, slots[mid]) + force(mid)
                if step == step_count - 1:
                    form(jnp.minimum(slab + 1, span - 1), 0, slots[0], 0, state_size)
                slope_four = apply_op(current + step_size * slope_three, slots[last]) + force(last)
                current = current + (step_size / 6.0) * (slope_one + 2.0 * slope_two + 2.0 * slope_three + slope_four)
            panels[pl.ds(slab, 1)] = current[None, :cols]
            responses[pl.ds(slab, 1)] = current[None, rows - 1:rows]
            ending[...] = current[rows - 1:rows]
            return current

        lax.fori_loop(0, span, slab_step, start)

    vmem = pl.BlockSpec(memory_space=pltpu.VMEM)
    square = (state_size, state_size)
    return pl.pallas_call(
        kernel,
        out_shape=[jax.ShapeDtypeStruct((span, count, state_size), full) for count in (cols, 1)]
        + [jax.ShapeDtypeStruct((1, state_size), full)],
        in_specs=[vmem] * 4,
        out_specs=[vmem] * 3,
        scratch_shapes=[pltpu.VMEM(square, full)] * 2 + [pltpu.VMEM(square, half)] * 6,
        compiler_params=pltpu.CompilerParams(vmem_limit_bytes=60 * 1024 * 1024),
    )


def partners(step):
    return [(i, i ^ step) for i in range(lax.axis_size("tm"))]


def team_gather(value, span, teams):
    if span & (span - 1):
        return lax.all_to_all(jnp.broadcast_to(value, (span,) + value.shape), "tm", 0, 0, axis_index_groups=teams)
    place = lax.axis_index("tm") % span
    values = [value] + [lax.ppermute(value, "tm", partners(step)) for step in range(1, span)]
    bit = 1
    while bit < span:
        is_upper = (place // bit) % 2 == 1
        values = [jnp.where(is_upper, values[k ^ bit], values[k]) for k in range(span)]
        bit *= 2
    return jnp.stack(values)


def team_sum(value, span, teams):
    if span & (span - 1):
        return jnp.sum(lax.all_to_all(value, "tm", 0, 0, axis_index_groups=teams), axis=0)
    place = lax.axis_index("tm") % span
    rows = [value[k] for k in range(span)]
    bit = 1
    while bit < span:
        is_upper = (place // bit) % 2 == 1
        rows = [jnp.where(is_upper, rows[k ^ bit], rows[k]) for k in range(span)]
        bit *= 2
    return rows[0] + sum(lax.ppermute(rows[step], "tm", partners(step)) for step in range(1, span))


def shards(initial_state, coupling, modulation, gains, forcing):
    state_size = coupling.shape[0]
    nodes = gains.shape[1]
    time_parts, col_parts = lax.axis_size("tm"), lax.axis_size("col")
    span = group_span(state_size, time_parts, col_parts)
    groups = time_parts // span
    members = span * col_parts
    cols = state_size // members
    time_index, col_index = lax.axis_index("tm"), lax.axis_index("col")
    group = time_index // span
    slab = time_index % span
    member = slab * col_parts + col_index
    teams = [[g * span + i for i in range(span)] for g in range(groups)]

    gain_row = jnp.pad(jnp.repeat(gains[0], 128), (0, state_size - nodes * 128))
    own = jnp.concatenate([forcing[0], gain_row[None]], axis=0)
    slab_data = team_gather(own, span, teams)

    panels, responses, ending = panel_kernel(state_size, nodes, span, cols)(coupling, modulation, initial_state[None], slab_data)

    if groups % 2 == 0:
        first_hop = [(i, i + span if i // span % 2 == 0 else i - span) for i in range(time_parts)]
    else:
        first_hop = [(i, (i + span) % time_parts) for i in range(time_parts)]
    arrived = lax.ppermute(ending, "tm", first_hop)
    begin = lax.dynamic_slice_in_dim(arrived[0], member * cols, cols, 0)
    begin = jnp.where(group == 1, begin, 0.0)
    source_group = jnp.arange(time_parts * col_parts).reshape(-1, 1, 1) // members
    for turn in range(1, groups - 1):
        partial = jnp.sum(panels[-1] * begin[:, None], axis=0)
        partial = partial + jnp.where(member == 0, ending[0], 0.0)
        outgoing = jnp.broadcast_to(partial.reshape(1, members, 1, cols), (groups, members, 1, cols)).reshape(-1, 1, cols)
        incoming = lax.all_to_all(outgoing, ("tm", "col"), 0, 0, tiled=True)
        summed = jnp.sum(jnp.where(source_group == group - 1, incoming, 0.0), axis=(0, 1))
        begin = jnp.where(group == turn + 1, summed, begin)

    partials = jnp.sum(panels * begin[None, :, None], axis=1)
    summed = team_sum(partials, span, teams).reshape(col_parts, state_size // col_parts)
    slab_end = lax.psum_scatter(summed, "col", scatter_dimension=0) if col_parts != 2 else (
        lax.dynamic_index_in_dim(summed, col_index, 0, False)
        + lax.ppermute(lax.dynamic_index_in_dim(summed, 1 - col_index, 0, False), "col", [(0, 1), (1, 0)])
    )
    own_response = lax.dynamic_index_in_dim(responses, slab, 0, False).reshape(col_parts, -1)
    slab_end = slab_end + lax.dynamic_index_in_dim(own_response, col_index, 0, False)
    return slab_end[None, :]


def solution(mesh):
    in_specs = (P(), P(), P(), P("tm", None), P("tm", None, None))
    out_specs = P("tm", "col")
    return jax.shard_map(shards, mesh=mesh, in_specs=in_specs, out_specs=out_specs, check_vma=False)
```
